16 devices in a mesh: rep: 1, dp: 16 (over x, y, z, core).
Axes of the slice: x: 2, y: 2, z: 2, core: 2. Of those that a mesh axis runs over, the one named last changes fastest.
Arguments:
- x: bfloat16 [16, 2048, 640], P(('rep', 'dp'))
- dy: bfloat16 [16, 2048, 640], P(('rep', 'dp'))
- wq: bfloat16 [2, 640, 640], replicated
- wk: bfloat16 [2, 640, 128], replicated
- wv: bfloat16 [2, 640, 128], replicated
- wo: bfloat16 [2, 640, 640], replicated
- w_gate: bfloat16 [2, 640, 3456], replicated
- w_up: bfloat16 [2, 640, 3456], replicated
- w_down: bfloat16 [2, 3456, 640], replicated
- m_wq: float32 [2, 640, 640], replicated
- m_wk: float32 [2, 640, 128], replicated
- m_wv: float32 [2, 640, 128], replicated
- m_wo: float32 [2, 640, 640], replicated
- m_w_gate: float32 [2, 640, 3456], replicated
- m_w_up: float32 [2, 640, 3456], replicated
- m_w_down: float32 [2, 3456, 640], replicated
- v_wq: float32 [2, 640, 640], replicated
- v_wk: float32 [2, 640, 128], replicated
- v_wv: float32 [2, 640, 128], replicated
- v_wo: float32 [2, 640, 640], replicated
- v_w_gate: float32 [2, 640, 3456], replicated
- v_w_up: float32 [2, 640, 3456], replicated
- v_w_down: float32 [2, 3456, 640], replicated
Outputs:
- output 1: bfloat16 [2, 640, 640], P('rep')
- output 2: bfloat16 [2, 640, 128], P('rep')
- output 3: bfloat16 [2, 640, 128], P('rep')
- output 4: bfloat16 [2, 640, 640], P('rep')
- output 5: bfloat16 [2, 640, 3456], P('rep')
- output 6: bfloat16 [2, 640, 3456], P('rep')
- output 7: bfloat16 [2, 3456, 640], P('rep')
- output 8: float32 [2, 640, 640], P('rep')
- output 9: float32 [2, 640, 128], P('rep')
- output 10: float32 [2, 640, 128], P('rep')
- output 11: float32 [2, 640, 640], P('rep')
- output 12: float32 [2, 640, 3456], P('rep')
- output 13: float32 [2, 640, 3456], P('rep')
- output 14: float32 [2, 3456, 640], P('rep')
- output 15: float32 [2, 640, 640], P('rep')
- output 16: float32 [2, 640, 128], P('rep')
- output 17: float32 [2, 640, 128], P('rep')
- output 18: float32 [2, 640, 640], P('rep')
- output 19: float32 [2, 640, 3456], P('rep')
- output 20: float32 [2, 640, 3456], P('rep')
- output 21: float32 [2, 3456, 640], P('rep')
All inputs are finite; a program needn't handle non-finite values.
Results may differ from the reference program's by a relative error of at most 0.024.
Values are sent between devices in bfloat16 or wider.
A program may use at most 2.5 GiB of HBM per device.

```python
import jax
import jax.numpy as jnp
from jax import lax

SEQUENCES = 16
TOKENS = 2048
D = 640
HEADS = 5
KV_HEADS = 1
HEAD = 128
FF = 3456
LAYERS = 2
THETA = 10000
NAMES = ("wq", "wk", "wv", "wo", "w_gate", "w_up", "w_down")
SHAPES = {
    "wq": (LAYERS, D, HEADS * HEAD),
    "wk": (LAYERS, D, KV_HEADS * HEAD),
    "wv": (LAYERS, D, KV_HEADS * HEAD),
    "wo": (LAYERS, HEADS * HEAD, D),
    "w_gate": (LAYERS, D, FF),
    "w_up": (LAYERS, D, FF),
    "w_down": (LAYERS, FF, D),
}


def bump(key, n, height):
    away = (jnp.arange(n, dtype=jnp.int32) - jax.random.randint(key, (), 0, n, jnp.int32)) % n
    return jnp.where(away < n // 8, height, 1.0)


def together(key, own, strength):
    shared = jax.random.normal(key, own.shape[1:], jnp.float32)
    return (own + strength * shared) * lax.rsqrt(1 + strength * strength)


def setup_inputs(seed: int = 0, part: int = 0) -> dict:
    kx, kdy, ka, kb, kz, kf, kh, kl, *keys = jax.random.split(jax.random.key(seed), 8 + 3 * len(NAMES))
    kx, kdy, ka, kb = (jax.random.fold_in(k, part) for k in (kx, kdy, ka, kb))
    kw, km, kv = (keys[i::3] for i in range(3))
    shape = (SEQUENCES, TOKENS, D)
    much_x, much_dy = jax.random.uniform(kz, (2,), jnp.float32, 0.0, 1.0)
    loud = 2.0 ** jax.random.uniform(jax.random.fold_in(kz, 1), (), jnp.float32, -1.0, 2.0)
    layers = 2.0 ** jax.random.uniform(kl, (LAYERS, 1, 1), jnp.float32, -1.0, 1.0)
    times = {"wq": 1.0, "wk": 1.0, "wv": 2.0, "wo": layers, "w_gate": 1.0, "w_up": bump(kh, FF, 4.0), "w_down": layers}
    x = together(ka, jax.random.normal(kx, shape, jnp.float32), much_x) * bump(kf, D, 4.0)
    dy = together(kb, jax.random.normal(kdy, shape, jnp.float32), much_dy)
    drawn = {"x": x.astype(jnp.bfloat16), "dy": (loud * dy * (SEQUENCES * TOKENS) ** -0.5).astype(jnp.bfloat16)}
    for key, name in zip(kw, NAMES, strict=True):
        drawn[name] = (jax.random.normal(key, SHAPES[name], jnp.float32) * SHAPES[name][1] ** -0.5 * times[name]).astype(jnp.bfloat16)
    for key, name in zip(km, NAMES, strict=True):
        drawn[f"m_{name}"] = 0.1 * jax.random.normal(key, SHAPES[name], jnp.float32)
    for key, name in zip(kv, NAMES, strict=True):
        drawn[f"v_{name}"] = jax.random.uniform(key, SHAPES[name], jnp.float32, 0.02, 0.06)
    return drawn


def matmul(a, w):
    return jnp.dot(a, w, preferred_element_type=jnp.float32).astype(jnp.bfloat16)


def normed(h):
    wide = h.astype(jnp.float32)
    scale = lax.rsqrt(jnp.mean(wide**2, -1, keepdims=True) + 1e-6)
    return (wide * scale).astype(jnp.bfloat16)


def turned(t, theta):
    half = t.shape[-1] // 2
    angle = jnp.arange(t.shape[0], dtype=jnp.float32)[:, None] * theta ** (-jnp.arange(half, dtype=jnp.float32) / half)
    cos, sin = jnp.cos(angle)[:, None], jnp.sin(angle)[:, None]
    a, b = t[..., :half].astype(jnp.float32), t[..., half:].astype(jnp.float32)
    return jnp.concatenate([a * cos - b * sin, b * cos + a * sin], -1).astype(jnp.bfloat16)


def seen_by(q, k, v):
    tokens, kv = q.shape[0], k.shape[1]
    q = q.reshape(tokens, kv, -1, q.shape[-1])
    scores = jnp.einsum("tgsd,ugd->gstu", q.astype(jnp.float32), k.astype(jnp.float32)) * q.shape[-1] ** -0.5
    place = jnp.arange(tokens)
    weights = jax.nn.softmax(jnp.where(place[:, None] >= place, scores, -jnp.inf), -1).astype(jnp.bfloat16)
    return jnp.einsum("gstu,ugd->tgsd", weights.astype(jnp.float32), v.astype(jnp.float32)).astype(jnp.bfloat16).reshape(tokens, -1)


def layer(h, w):
    a = normed(h)
    q, k = (turned(matmul(a, w[name]).reshape(h.shape[0], -1, HEAD), THETA) for name in ("wq", "wk"))
    h = h + matmul(seen_by(q, k, matmul(a, w["wv"]).reshape(h.shape[0], -1, HEAD)), w["wo"])
    b = normed(h)
    gate = jnp.dot(b, w["w_gate"], preferred_element_type=jnp.float32)
    up = jnp.dot(b, w["w_up"], preferred_element_type=jnp.float32)
    return h + matmul((jax.nn.silu(gate) * up).astype(jnp.bfloat16), w["w_down"])


def adamw(w, m, v, g):
    m = 0.9 * m + 0.1 * g
    v = 0.95 * v + 0.05 * g * g
    step = m * lax.rsqrt(v + 1e-8) + 0.1 * w
    return (w - 0.02 * step).astype(jnp.bfloat16), m, v


def clipped(gradients, sum_of_squares, count):
    factor = jnp.minimum(1.0, 0.5 * lax.rsqrt(sum_of_squares / count + 1e-30))
    return [g * factor for g in gradients]


def stack(weights, h):
    return lax.scan(lambda h, w: (layer(h, w), None), h, weights)[0]


def reference(x, dy, wq, wk, wv, wo, w_gate, w_up, w_down, m_wq, m_wk, m_wv, m_wo, m_w_gate, m_w_up, m_w_down, v_wq, v_wk, v_wv, v_wo, v_w_gate, v_w_up, v_w_down):
    weights = dict(zip(NAMES, (wq, wk, wv, wo, w_gate, w_up, w_down), strict=True))

    def take(so_far, sequence):
        h, by_y = sequence
        _, back = jax.vjp(stack, weights, h)
        by_weights, by_h = back(by_y)
        return jax.tree.map(lambda total, term: total + term.astype(jnp.float32), so_far, by_weights), by_h

    none_yet = {name: jnp.zeros(w.shape, jnp.float32) for name, w in weights.items()}
    by_weights, by_x = lax.scan(take, none_yet, (x, dy))
    gradients = [by_weights[name].astype(jnp.bfloat16).astype(jnp.float32) for name in NAMES]
    gradients = clipped(gradients, sum(jnp.sum(g * g) for g in gradients), sum(g.size for g in gradients))
    first = (m_wq, m_wk, m_wv, m_wo, m_w_gate, m_w_up, m_w_down)
    second = (v_wq, v_wk, v_wv, v_wo, v_w_gate, v_w_up, v_w_down)
    new = [adamw(weights[name].astype(jnp.float32), m, v, g) for name, m, v, g in zip(NAMES, first, second, gradients, strict=True)]
    return tuple(one[which] for which in range(3) for one in new)
```

```python
import functools

import jax
import jax.numpy as jnp
from jax import lax
from jax.experimental import pallas as pl
from jax.experimental.pallas import tpu as pltpu
from jax.sharding import PartitionSpec as P

NEG = -1e30
HIDDEN = 2 * NEG
LOG2E = 1.4426950408889634
HEAD = 128
THETA = 10000
VMEM = 60 * 2**20
STRIP = 512
ALL = ...
BF = jnp.bfloat16
F32 = jnp.float32
NN, NT, TN = (1, 0), (1, 1), (0, 0)

UPDATE_BLOCKS = (5, 5, 6)


def _dot(a, b, ca, cb):
    return lax.dot_general(a, b, (((ca,), (cb,)), ((), ())), preferred_element_type=F32)


def _params(*kinds):
    return pltpu.CompilerParams(dimension_semantics=kinds, vmem_limit_bytes=VMEM)


def _cost(flops, *arrays):
    return pl.CostEstimate(flops=int(flops), transcendentals=0, bytes_accessed=sum(a.size * a.dtype.itemsize for a in arrays))


def _once(shape, index):
    return pl.BlockSpec(shape, index, pipeline_mode=pl.Buffered(1))


def _turn(t, cos, sin):
    return t * cos + pltpu.roll(t, HEAD // 2, 1) * sin


def _scale_of(x):
    return lax.rsqrt(jnp.mean(x * x, -1, keepdims=True) + 1e-6)


def _norm_back(x, d):
    s = _scale_of(x)
    return s * d - x * (s * s * s * jnp.mean(d * x, -1, keepdims=True))


ORDERS = ((1, 8, 4, 2), (1, 4, 2, 8), (1, 2, 8, 4))
BITS = (1, 2, 4, 8)
TILE = (8, 128)
MESH = pl.DeviceIdType.MESH


def _bit(me, bit):
    return lax.rem(lax.div(me, bit), 2)


def _partner(me, bit):
    return {"dp": me + bit * (1 - 2 * _bit(me, bit))}


def _greet(me):
    barrier = pltpu.get_barrier_semaphore()
    for bit in BITS:
        pl.semaphore_signal(barrier, device_id=_partner(me, bit), device_id_type=MESH)
    pl.semaphore_wait(barrier, len(BITS))


def _squares(x):
    x = x.astype(F32)
    x = (x * x).sum(axis=0, keepdims=True)
    return sum(x[:, at : at + TILE[1]] for at in range(0, x.shape[1], TILE[1]))


class Exchanges:
    def __init__(self, me, streams, mine, buffers, send, recv, local, outs=None):
        self.me, self.streams, self.mine, self.buffers, self.outs = me, streams, mine, buffers, outs
        self.send, self.recv, self.local = send, recv, local
        self.bits = [[_bit(me, bit) for bit in ORDERS[s[2]]] for s in streams]

    def inside(self, n, phase):
        made = max(self.streams[n][3], 1)
        return sum((16 >> (i + 1)) * self.bits[n][i] for i in range(made, phase))

    def block(self, n, phase=4):
        return sum((16 >> (i + 1)) * self.bits[n][i] for i in range(phase))

    def copy(self, n, phase):
        array, columns, group, made = self.streams[n]
        keep, *came = self.buffers[n]
        if phase < 4:
            half = 8 >> phase
            if phase == 0:
                source = self.mine[array].at[pl.ds(half * (1 - self.bits[n][0]), half), :, columns]
            else:
                source = keep.at[pl.ds(self.inside(n, phase) + half * (1 - self.bits[n][phase]), half)]
            target, bit = came[phase - made], ORDERS[group][phase]
        else:
            here = pl.ds(self.block(n, 8 - phase), 1 << (phase - 4))
            source, bit = came[-1].at[here], ORDERS[group][7 - phase]
            target = self.outs[array].at[here, :, columns] if phase == 7 else source
        return pltpu.make_async_remote_copy(src_ref=source, dst_ref=target, send_sem=self.send.at[n, phase], recv_sem=self.recv.at[n, phase],
                                            device_id=_partner(self.me, bit), device_id_type=MESH)

    def load(self, n):
        array, columns, _, made = self.streams[n]
        source = self.mine[array].at[:, :, columns] if made else self.mine[array].at[pl.ds(8 * self.bits[n][0], 8), :, columns]
        return pltpu.make_async_copy(source, self.buffers[n][0], self.local.at[n])

    def store(self, n):
        array, columns, _, _ = self.streams[n]
        here = pl.ds(self.block(n, 1), 8)
        return pltpu.make_async_copy(self.buffers[n][-1].at[here], self.outs[array].at[here, :, columns], self.local.at[n])

    def begin(self, n):
        if not self.streams[n][3]:
            self.copy(n, 0).start()
        self.load(n).start()

    def take(self, n, phase):
        made = self.streams[n][3]
        if phase == made:
            self.load(n).wait()
        self.copy(n, phase).wait_recv()
        keep, came = self.buffers[n][0], self.buffers[n][1 + phase - made]
        at = self.inside(n, phase + 1)

        def one(i, _):
            keep[at + i] = (keep[at + i].astype(F32) + came[i].astype(F32)).astype(BF)

        lax.fori_loop(0, 8 >> phase, one, None)


def _streams(views, groups, made):
    streams = []
    for array, view in enumerate(views):
        rows, width = view.shape[1:]
        cut = width if width * rows < 2**16 else -(-width // 256) * 128
        streams += [(array, slice(at, min(at + cut, width)), groups[array], made[array]) for at in range(0, width, cut)]
    return sorted(streams, key=lambda s: (s[1].start, -views[s[0]].size))


def _blocks_of(g):
    return g.reshape(16, g.shape[0] // 16, g.shape[1])


def _sync_kernel(*refs, streams, many, more):
    mine, others, outs, total = refs[:many], refs[many : many + more], refs[many + more : 2 * many + more], refs[2 * many + more]
    scratch = list(refs[2 * many + more + 1 :])
    blocks = [scratch.pop(0) for _ in range(more)]
    buffers = [[scratch.pop(0) for _ in range(2 + 4 - s[3])] for s in streams]
    sums, send, recv, local, sum_send, sum_recv, block_sem = scratch
    me = lax.axis_index("dp")
    _greet(me)
    x = Exchanges(me, streams, mine, buffers, send, recv, local, outs)
    every = range(len(streams))
    ready = [n for n in every if streams[n][3]]
    fresh = [n for n in every if not streams[n][3]]
    for n in fresh + ready:
        x.begin(n)
    loads = []
    for array in range(more):
        n = [s[0] for s in streams].index(array)
        loads.append(pltpu.make_async_copy(others[array].at[x.block(n)], blocks[array], block_sem.at[array]))
        loads[-1].start()
    for n in ready:
        x.load(n).wait()
        x.copy(n, 3).start()
    part = jnp.zeros((1, TILE[1]), F32)
    for load, block in zip(loads, blocks):
        load.wait()
        part = part + _squares(block[ALL])
    for phase in range(3):
        for n in fresh:
            x.take(n, phase)
            x.copy(n, phase + 1).start()
    for n in ready + fresh:
        keep, came, whole = buffers[n][0], buffers[n][-2], buffers[n][-1]
        x.copy(n, 3).wait_recv()
        summed = (keep[x.inside(n, 4)].astype(F32) + came[0].astype(F32)).astype(BF)
        whole[x.block(n)] = summed
        part = part + _squares(summed)
        x.copy(n, 4).start()
    sums[0] = jnp.broadcast_to(part, TILE)
    sum_copies = []
    for step, bit in enumerate(BITS):
        sum_copies.append(pltpu.make_async_remote_copy(src_ref=sums.at[2 * step], dst_ref=sums.at[2 * step + 1], send_sem=sum_send.at[step],
                                                       recv_sem=sum_recv.at[step], device_id=_partner(me, bit), device_id_type=MESH))
        sum_copies[step].start()
        if step < 3:
            for n in ready + fresh:
                x.copy(n, 4 + step).wait_recv()
                x.copy(n, 5 + step).start()
                if step == 2:
                    x.store(n).start()
        sum_copies[step].wait_recv()
        sums[2 * step + 2] = sums[2 * step] + sums[2 * step + 1]
    total[ALL] = sums[2 * len(BITS)]
    for n in every:
        x.copy(n, 7).wait_recv()
        x.store(n).wait()
        for phase in range(streams[n][3], 8):
            x.copy(n, phase).wait_send()
    for copy in sum_copies:
        copy.wait_send()


def synchronize(mine, others, groups, made):
    many, more = len(mine), len(others)
    streams = _streams(mine, groups, made)
    scratch = [pltpu.VMEM(v.shape[1:], BF) for v in others]
    for array, columns, _, done in streams:
        first = 16 >> max(done, 1)
        counts = [first] + [8 >> phase for phase in range(done, 4)] + [16]
        scratch += [pltpu.VMEM((count, mine[array].shape[1], columns.stop - columns.start), BF) for count in counts]
    sems = pltpu.SemaphoreType.DMA
    count = len(streams)
    hbm = pl.BlockSpec(memory_space=pl.ANY)
    *outs, total = pl.pallas_call(
        functools.partial(_sync_kernel, streams=streams, many=many, more=more),
        in_specs=[hbm] * (many + more),
        out_specs=[hbm] * many + [pl.BlockSpec(memory_space=pltpu.VMEM)],
        out_shape=[jax.ShapeDtypeStruct((16, *v.shape[1:]), BF) for v in mine] + [jax.ShapeDtypeStruct(TILE, F32)],
        scratch_shapes=scratch + [pltpu.VMEM((2 * len(BITS) + 1, *TILE), F32), sems((count, 8)), sems((count, 8)), sems((count,)),
                                  sems((4,)), sems((4,)), sems((more,))],
        compiler_params=pltpu.CompilerParams(collective_id=0, has_side_effects=True, vmem_limit_bytes=VMEM),
        cost_estimate=_cost(10**9, *mine),
        name="synchronize",
    )(*mine, *others)
    return [o.reshape(-1, o.shape[2]) for o in outs], total


def _pre_kernel(h_ref, wq_ref, wk_ref, wv_ref, cos_ref, sin_ref, a_ref, q_ref, k_ref, v_ref):
    x = h_ref[ALL].astype(F32)
    a = (x * _scale_of(x)).astype(BF)
    a_ref[ALL] = a
    cos, sin = cos_ref[ALL], sin_ref[ALL]

    def turned(t):
        return _turn(t.astype(BF).astype(F32), cos, sin).astype(BF)

    q = _dot(a, wq_ref[ALL], *NN)
    for n in range(q.shape[1] // HEAD):
        q_ref[:, n * HEAD : (n + 1) * HEAD] = turned(q[:, n * HEAD : (n + 1) * HEAD])
    k_ref[ALL] = turned(_dot(a, wk_ref[ALL], *NN))
    v_ref[ALL] = _dot(a, wv_ref[ALL], *NN).astype(BF)


def pre(h, wq, wk, wv, layer, cos, sin, bt=512):
    t, d = h.shape
    rows = lambda w: pl.BlockSpec((bt, w), lambda i: (i, 0))
    weight = lambda w: pl.BlockSpec((None, *w.shape[1:]), lambda i: (layer, 0, 0))
    return pl.pallas_call(
        _pre_kernel,
        grid=(t // bt,),
        in_specs=[rows(d), weight(wq), weight(wk), weight(wv), rows(HEAD), rows(HEAD)],
        out_specs=[rows(d), rows(wq.shape[2]), rows(HEAD), rows(HEAD)],
        out_shape=[jax.ShapeDtypeStruct((t, w), BF) for w in (d, wq.shape[2], HEAD, HEAD)],
        compiler_params=_params("parallel"),
        cost_estimate=_cost(2 * t * d * (wq.shape[2] + 2 * HEAD), h, h, h, h),
        name="attn_pre",
    )(h, wq, wk, wv, cos, sin)


def _gap(bk, cols, bq):
    return lax.rem(lax.broadcasted_iota(jnp.int32, (bk, cols), 1), bq) - lax.broadcasted_iota(jnp.int32, (bk, cols), 0)


def _pieces(g, bq):
    wide = min(STRIP, bq)
    return wide, [(n, at, n * bq + at) for n in range(g) for at in range(0, bq, wide)]


def _attend_kernel(q_ref, k_ref, v_ref, o_ref, lse_ref, top_s, mix_s, gap_s, *, scale, bk):
    bq, g = q_ref.shape[0], q_ref.shape[1] // HEAD
    cols = g * bq
    iq = pl.program_id(0)
    e = scale * LOG2E
    wide, pieces = _pieces(g, bq)

    @pl.when(iq == 0)
    def _():
        gap_s[ALL] = _gap(bk, cols, bq)

    top_s[ALL] = jnp.full((1, cols), NEG, F32)
    mix_s[ALL] = jnp.zeros((HEAD + 8, cols), F32)
    ones = jnp.ones((8, bk), BF)

    def block(j, masked):
        here = pl.ds(pl.multiple_of(j * bk, bk), bk)
        keys = k_ref[here, :]
        scores = [_dot(keys, q_ref[at : at + wide, n * HEAD : (n + 1) * HEAD], *NT) for n, at, _ in pieces]
        weights, keeps = [], []
        for (n, at, c), s in zip(pieces, scores):
            if masked:
                s = jnp.where(gap_s[:, c : c + wide] >= j * bk - iq * bq, s, HIDDEN)
            old = top_s[:, c : c + wide]
            top = jnp.maximum(old, s.max(axis=0, keepdims=True))
            top_s[:, c : c + wide] = top
            weights.append(jnp.exp2((s - top) * e).astype(BF))
            keeps.append(jnp.exp2((old - top) * e))
        values = jnp.concatenate([v_ref[here, :].T, ones], axis=0)
        for (n, at, c), p, keep in zip(pieces, weights, keeps):
            mix_s[:, c : c + wide] = mix_s[:, c : c + wide] * keep + _dot(values, p, *NN)

    whole = lax.div(iq * bq + 1, bk)
    last = lax.div(iq * bq + bq - 1 + bk, bk)
    lax.fori_loop(0, whole, lambda j, _: block(j, False), None)
    lax.fori_loop(whole, last, lambda j, _: block(j, True), None)
    total = mix_s[HEAD : HEAD + 1, :]
    lse = top_s[ALL] * scale + jnp.log(total)
    inv = 1 / total
    for n in range(g):
        c = n * bq
        o_ref[:, n * HEAD : (n + 1) * HEAD] = (mix_s[:HEAD, c : c + bq] * inv[:, c : c + bq]).T.astype(BF)
        lse_ref[n : n + 1, :] = lse[:, c : c + bq]


def attend(q, k, v, bq=512, bk=512):
    t, hd = q.shape
    g = hd // HEAD
    every = pl.BlockSpec((t, HEAD), lambda i: (0, 0))
    return pl.pallas_call(
        functools.partial(_attend_kernel, scale=HEAD**-0.5, bk=bk),
        grid=(t // bq,),
        in_specs=[pl.BlockSpec((bq, hd), lambda i: (i, 0)), every, every],
        out_specs=[pl.BlockSpec((bq, hd), lambda i: (i, 0)), pl.BlockSpec((g, bq), lambda i: (0, i))],
        out_shape=[jax.ShapeDtypeStruct((t, hd), BF), jax.ShapeDtypeStruct((g, t), F32)],
        scratch_shapes=[pltpu.VMEM((1, g * bq), F32), pltpu.VMEM((HEAD + 8, g * bq), F32), pltpu.VMEM((bk, g * bq), jnp.int32)],
        compiler_params=_params("arbitrary"),
        cost_estimate=_cost(8 * g * t * t * HEAD, q, k, v, q),
        name="attend",
    )(q, k, v)


def _attend_bwd_kernel(q_ref, k_ref, v_ref, o_ref, do_ref, lse_ref, cosq_ref, sinq_ref, cos_ref, sin_ref, dq_ref, dk_ref, dv_ref,
                       dq_s, dk_s, dv_s, gap_s, *, scale, bk, hook=None):
    bq, g = q_ref.shape[0], q_ref.shape[1] // HEAD
    cols = g * bq
    iq = pl.program_id(0)
    e = scale * LOG2E
    wide, pieces = _pieces(g, bq)

    @pl.when(iq == 0)
    def _():
        gap_s[ALL] = _gap(bk, cols, bq)
        dk_s[ALL] = jnp.zeros_like(dk_s)
        dv_s[ALL] = jnp.zeros_like(dv_s)

    if hook:
        hook(iq, False)
    dq_s[ALL] = jnp.zeros_like(dq_s)
    lses = [lse_ref[n : n + 1, at : at + wide] * LOG2E for n, at, _ in pieces]
    deltas = []
    for n, at, _ in pieces:
        product = do_ref[at : at + wide, n * HEAD : (n + 1) * HEAD].astype(F32) * o_ref[at : at + wide, n * HEAD : (n + 1) * HEAD].astype(F32)
        deltas.append(product.T.sum(axis=0, keepdims=True))

    def block(j, masked):
        here = pl.ds(pl.multiple_of(j * bk, bk), bk)
        keys, values = k_ref[here, :], v_ref[here, :]
        qs = [q_ref[at : at + wide, n * HEAD : (n + 1) * HEAD] for n, at, _ in pieces]
        dos = [do_ref[at : at + wide, n * HEAD : (n + 1) * HEAD] for n, at, _ in pieces]
        scores = [_dot(keys, x, *NT) for x in qs]
        dps = [_dot(values, x, *NT) for x in dos]
        keys_t = keys.T
        for i, (n, at, c) in enumerate(pieces):
            p = jnp.exp2(scores[i] * e - lses[i])
            if masked:
                p = jnp.where(gap_s[:, c : c + wide] >= j * bk - iq * bq, p, 0.0)
            ds = (p * (dps[i] - deltas[i])).astype(BF)
            dv_s[here, :] += _dot(p.astype(BF), dos[i], *NN)
            dk_s[here, :] += _dot(ds, qs[i], *NN)
            dq_s[:, c : c + wide] += _dot(keys_t, ds, *NN)

    whole = lax.div(iq * bq + 1, bk)
    last = lax.div(iq * bq + bq - 1 + bk, bk)
    lax.fori_loop(0, whole, lambda j, _: block(j, False), None)
    lax.fori_loop(whole, last, lambda j, _: block(j, True), None)
    for n in range(g):
        d = (dq_s[:, n * bq : (n + 1) * bq] * scale).T.astype(BF).astype(F32)
        dq_ref[:, n * HEAD : (n + 1) * HEAD] = _turn(d, cosq_ref[ALL], -sinq_ref[ALL]).astype(BF)

    @pl.when(iq == pl.num_programs(0) - 1)
    def _():
        d = (dk_s[ALL] * scale).astype(BF).astype(F32)
        dk_ref[ALL] = _turn(d, cos_ref[ALL], -sin_ref[ALL]).astype(BF)
        dv_ref[ALL] = dv_s[ALL].astype(BF)

    if hook:
        hook(iq, True)


def _attend_bwd_sync_kernel(*refs, streams, many, scale, bk):
    given, mine, results, lefts, scratch = refs[:10], refs[10 : 10 + many], refs[10 + many : 13 + many], refs[13 + many : 13 + 2 * many], refs[13 + 2 * many :]
    own, scratch = scratch[:4], list(scratch[4:])
    buffers = [[scratch.pop(0) for _ in range(4)] for _ in streams]
    me = lax.axis_index("dp")
    x = Exchanges(me, streams, mine, buffers, *scratch)
    every = range(len(streams))
    early = [n for n in every if n < 3]
    late = [n for n in every if n >= 3]

    def hook(step, after):
        if after:

            @pl.when(step == HOOKS[3])
            def _():
                for n in every:
                    array, columns, _, _ = streams[n]
                    x.take(n, 2)
                    lefts[array][:, :, columns] = buffers[n][0][pl.ds(x.inside(n, 3), 2)]
                for n in every:
                    for phase in range(3):
                        x.copy(n, phase).wait_send()

            return

        @pl.when(step == 0)
        def _():
            _greet(me)
            for n in every:
                x.begin(n)

        for place, phase, some in ((0, 0, early), (1, 0, late), (2, 1, every)):

            @pl.when(step == HOOKS[place])
            def _(phase=phase, some=some):
                for n in some:
                    x.take(n, phase)
                    x.copy(n, phase + 1).start()

    _attend_bwd_kernel(*given, *results, *own, scale=scale, bk=bk, hook=hook)


HOOKS = (3, 4, 7, 7)


def attend_bwd(q, k, v, o, do, lse, cos, sin, mine=(), groups=(), bq=256, bk=512):
    t, hd = q.shape
    g = hd // HEAD
    every = pl.BlockSpec((t, HEAD), lambda i: (0, 0))
    some = pl.BlockSpec((bq, hd), lambda i: (i, 0))
    table = pl.BlockSpec((bq, HEAD), lambda i: (i, 0))
    kernel, name, params, many = functools.partial(_attend_bwd_kernel, scale=HEAD**-0.5, bk=bk), "attend_bwd", _params("arbitrary"), len(mine)
    scratch = [pltpu.VMEM((HEAD, g * bq), F32), pltpu.VMEM((t, HEAD), F32), pltpu.VMEM((t, HEAD), F32), pltpu.VMEM((bk, g * bq), jnp.int32)]
    if mine:
        streams = _streams(mine, groups, [0] * many)
        kernel = functools.partial(_attend_bwd_sync_kernel, streams=streams, many=many, scale=HEAD**-0.5, bk=bk)
        name = "attend_bwd_sync"
        params = pltpu.CompilerParams(dimension_semantics=("arbitrary",), collective_id=1, has_side_effects=True, vmem_limit_bytes=VMEM)
        for array, columns, _, _ in streams:
            scratch += [pltpu.VMEM((count, mine[array].shape[1], columns.stop - columns.start), BF) for count in (8, 8, 4, 2)]
        sems = pltpu.SemaphoreType.DMA
        scratch += [sems((len(streams), 3)), sems((len(streams), 3)), sems((len(streams),))]
    lefts = [jax.ShapeDtypeStruct((2, *g.shape[1:]), BF) for g in mine]
    return pl.pallas_call(
        kernel,
        grid=(t // bq,),
        in_specs=[some, every, every, some, some, pl.BlockSpec((g, bq), lambda i: (0, i)), table, table, every, every]
        + [pl.BlockSpec(memory_space=pl.ANY)] * many,
        out_specs=[some, every, every] + [_once(left.shape, lambda i: (0, 0, 0)) for left in lefts],
        out_shape=[jax.ShapeDtypeStruct((t, w), BF) for w in (hd, HEAD, HEAD)] + lefts,
        scratch_shapes=scratch,
        compiler_params=params,
        cost_estimate=_cost(14 * g * t * t * HEAD, q, q, q, q),
        name=name,
    )(q, k, v, o, do, lse, cos, sin, cos, sin, *mine)


def _post_kernel(o_ref, wo_ref, h_ref, mid_ref, b_ref):
    mid = h_ref[ALL] + _dot(o_ref[ALL], wo_ref[ALL], *NN).astype(BF)
    mid_ref[ALL] = mid
    x = mid.astype(F32)
    b_ref[ALL] = (x * _scale_of(x)).astype(BF)


def post(o, wo, layer, h, bt=512):
    t, d = h.shape
    rows = lambda w: pl.BlockSpec((bt, w), lambda i: (i, 0))
    return pl.pallas_call(
        _post_kernel,
        grid=(t // bt,),
        in_specs=[rows(o.shape[1]), pl.BlockSpec((None, *wo.shape[1:]), lambda i: (layer, 0, 0)), rows(d)],
        out_specs=[rows(d), rows(d)],
        out_shape=[jax.ShapeDtypeStruct((t, d), BF)] * 2,
        compiler_params=_params("parallel"),
        cost_estimate=_cost(2 * t * d * d, h, h, h, h),
        name="attn_post",
    )(o, wo, h)


def _post_bwd_kernel(db_ref, mid_ref, dh_ref, o_ref, wo_ref, dmid_ref, do_ref, dwo_ref, acc):
    i = pl.program_id(0)
    dx = _norm_back(mid_ref[ALL].astype(F32), db_ref[ALL].astype(F32)).astype(BF)
    dmid = dh_ref[ALL] + dx
    dmid_ref[ALL] = dmid
    do_ref[ALL] = _dot(dmid, wo_ref[ALL], *NT).astype(BF)
    part = _dot(o_ref[ALL], dmid, *TN)

    @pl.when(i == 0)
    def _():
        acc[ALL] = part

    @pl.when(i > 0)
    def _():
        acc[ALL] += part

    @pl.when(i == pl.num_programs(0) - 1)
    def _():
        dwo_ref[ALL] = acc[ALL].astype(BF)


def post_bwd(db, mid, dh, o, wo, layer, bt=512):
    t, d = dh.shape
    rows = lambda w: pl.BlockSpec((bt, w), lambda i: (i, 0))
    return pl.pallas_call(
        _post_bwd_kernel,
        grid=(t // bt,),
        in_specs=[rows(d), rows(d), rows(d), rows(o.shape[1]), pl.BlockSpec((None, *wo.shape[1:]), lambda i: (layer, 0, 0))],
        out_specs=[rows(d), rows(o.shape[1]), pl.BlockSpec(wo.shape[1:], lambda i: (0, 0))],
        out_shape=[jax.ShapeDtypeStruct((t, d), BF), jax.ShapeDtypeStruct(o.shape, BF), jax.ShapeDtypeStruct(wo.shape[1:], BF)],
        scratch_shapes=[pltpu.VMEM(wo.shape[1:], F32)],
        compiler_params=_params("arbitrary"),
        cost_estimate=_cost(4 * t * d * d, dh, dh, dh, dh, dh, dh),
        name="attn_post_bwd",
    )(db, mid, dh, o, wo)


def _pre_bwd_kernel(dq_ref, dk_ref, dv_ref, a_ref, *rest, further):
    if further:
        h_ref, dmid_ref, wq_ref, wk_ref, wv_ref, dwq_ref, dwkv_ref, dh_ref, acc = rest
    else:
        dwq_ref, dwkv_ref, acc = rest
    i = pl.program_id(0)
    dq, dk, dv = dq_ref[ALL], dk_ref[ALL], dv_ref[ALL]
    part = _dot(a_ref[ALL], jnp.concatenate([dq, dk, dv], axis=1), *TN)

    @pl.when(i == 0)
    def _():
        acc[ALL] = part

    @pl.when(i > 0)
    def _():
        acc[ALL] += part

    @pl.when(i == pl.num_programs(0) - 1)
    def _():
        wide = dwq_ref.shape[1]
        dwq_ref[ALL] = acc[:, :wide].astype(BF)
        dwkv_ref[ALL] = acc[:, wide:].astype(BF)

    if further:
        da = (_dot(dq, wq_ref[ALL], *NT) + _dot(dk, wk_ref[ALL], *NT) + _dot(dv, wv_ref[ALL], *NT)).astype(BF).astype(F32)
        dh_ref[ALL] = dmid_ref[ALL] + _norm_back(h_ref[ALL].astype(F32), da).astype(BF)


def pre_bwd(dq, dk, dv, a, h, dmid, wq, wk, wv, layer, further, bt=512):
    t, d = a.shape
    wide = dq.shape[1]
    rows = lambda w: pl.BlockSpec((bt, w), lambda i: (i, 0))
    weight = lambda w: pl.BlockSpec((None, *w.shape[1:]), lambda i: (layer, 0, 0))
    given = [dq, dk, dv, a]
    specs = [rows(wide), rows(HEAD), rows(HEAD), rows(d)]
    outs = [jax.ShapeDtypeStruct((d, wide), BF), jax.ShapeDtypeStruct((d, 2 * HEAD), BF)]
    out_specs = [pl.BlockSpec(s.shape, lambda i: (0, 0)) for s in outs]
    if further:
        given += [h, dmid, wq, wk, wv]
        specs += [rows(d), rows(d), weight(wq), weight(wk), weight(wv)]
        outs.append(jax.ShapeDtypeStruct((t, d), BF))
        out_specs.append(rows(d))
    return pl.pallas_call(
        functools.partial(_pre_bwd_kernel, further=further),
        grid=(t // bt,),
        in_specs=specs,
        out_specs=out_specs,
        out_shape=outs,
        scratch_shapes=[pltpu.VMEM((d, wide + 2 * HEAD), F32)],
        compiler_params=_params("arbitrary"),
        cost_estimate=_cost((4 if further else 2) * t * d * (wide + 2 * HEAD), a, a, a, a),
        name="attn_pre_bwd",
    )(*given)


def _silu(g):
    s = 1 / (1 + jnp.exp(-g))
    return s, g * s


def _ff_kernel(b_ref, mid_ref, wg_ref, wu_ref, wd_ref, out_ref, *, chunk):
    b = b_ref[ALL]
    width = wg_ref.shape[1]
    total = None
    for at in range(0, width, chunk):
        f = slice(at, min(at + chunk, width))
        _, s = _silu(_dot(b, wg_ref[:, f], *NN))
        act = (s * _dot(b, wu_ref[:, f], *NN)).astype(BF)
        part = _dot(act, wd_ref[f, :], *NN)
        total = part if total is None else total + part
    out_ref[ALL] = mid_ref[ALL] + total.astype(BF)


def ff(b, mid, wg, wu, wd, layer, bt=512, chunk=768):
    t, d = b.shape
    rows = pl.BlockSpec((bt, d), lambda i: (i, 0))
    weight = lambda w: _once((None, *w.shape[1:]), lambda i: (layer, 0, 0))
    return pl.pallas_call(
        functools.partial(_ff_kernel, chunk=chunk),
        grid=(t // bt,),
        in_specs=[rows, rows, weight(wg), weight(wu), weight(wd)],
        out_specs=rows,
        out_shape=jax.ShapeDtypeStruct((t, d), BF),
        compiler_params=_params("parallel"),
        cost_estimate=_cost(6 * t * d * wg.shape[2], b, b, b, wg, wu),
        name="ff",
    )(b, mid, wg, wu, wd)


def _ff_bwd_kernel(b_ref, dh_ref, wg_ref, wu_ref, wd_ref, dwg_ref, dwu_ref, dwd_ref, db_ref, bt_s, dht_s, act_s, dg_s, du_s, acc, *, width, tb):
    j = pl.program_id(0)
    t, block = b_ref.shape[0], wg_ref.shape[1]
    left = width - j * block

    @pl.when(j == 0)
    def _():
        bt_s[ALL] = b_ref[ALL].T
        dht_s[ALL] = dh_ref[ALL].T
        acc[ALL] = jnp.zeros_like(acc)

    across = lax.broadcasted_iota(jnp.int32, (1, block), 1) < left
    down = lax.broadcasted_iota(jnp.int32, (block, 1), 0) < left
    zero = jnp.zeros((), BF)
    wg, wu, wd = jnp.where(across, wg_ref[ALL], zero), jnp.where(across, wu_ref[ALL], zero), jnp.where(down, wd_ref[ALL], zero)
    for at in range(0, t, tb):
        here = slice(at, at + tb)
        b, dh = b_ref[here, :], dh_ref[here, :]
        g, u = _dot(b, wg, *NN), _dot(b, wu, *NN)
        da = _dot(dh, wd, *NT).astype(BF).astype(F32)
        s, silu = _silu(g)
        act_s[here, :] = (silu * u).astype(BF)
        du = (da * silu).astype(BF)
        dg = (da * u * (s + silu * (1 - s))).astype(BF)
        du_s[here, :] = du
        dg_s[here, :] = dg
        acc[here, :] += _dot(dg, wg, *NT) + _dot(du, wu, *NT)
    dwg_ref[ALL] = _dot(bt_s[ALL], dg_s[ALL], *NN).astype(BF)
    dwu_ref[ALL] = _dot(bt_s[ALL], du_s[ALL], *NN).astype(BF)
    dwd_ref[ALL] = _dot(dht_s[ALL], act_s[ALL], *NN).T.astype(BF)

    @pl.when(j == pl.num_programs(0) - 1)
    def _():
        db_ref[ALL] = acc[ALL].astype(BF)


def ff_bwd(b, dh, wg, wu, wd, layer, block=512, tb=512):
    t, d = b.shape
    width = wg.shape[2]
    every = _once((t, d), lambda j: (0, 0))
    columns = pl.BlockSpec((None, d, block), lambda j: (layer, 0, j))
    out_columns = pl.BlockSpec((d, block), lambda j: (0, j))
    return pl.pallas_call(
        functools.partial(_ff_bwd_kernel, width=width, tb=tb),
        grid=(-(-width // block),),
        in_specs=[every, every, columns, columns, pl.BlockSpec((None, block, d), lambda j: (layer, j, 0))],
        out_specs=[out_columns, out_columns, pl.BlockSpec((block, d), lambda j: (j, 0)), _once((t, d), lambda j: (0, 0))],
        out_shape=[jax.ShapeDtypeStruct((d, width), BF), jax.ShapeDtypeStruct((d, width), BF), jax.ShapeDtypeStruct((width, d), BF),
                   jax.ShapeDtypeStruct((t, d), BF)],
        scratch_shapes=[pltpu.VMEM((d, t), BF), pltpu.VMEM((d, t), BF)] + [pltpu.VMEM((t, block), BF)] * 3 + [pltpu.VMEM((t, d), F32)],
        compiler_params=_params("arbitrary"),
        cost_estimate=_cost(16 * t * d * width, b, dh, wg, wu, wd),
        name="ff_bwd",
    )(b, dh, wg, wu, wd)


def adamw(w, m, v, g):
    m = 0.9 * m + 0.1 * g
    v = 0.95 * v + 0.05 * g * g
    step = m * lax.rsqrt(v + 1e-8) + 0.1 * w
    return (w - 0.02 * step).astype(BF), m, v


def _update_kernel(factor_ref, w_ref, m_ref, v_ref, *rest):
    gs, (w_out, m_out, v_out) = rest[:-3], rest[-3:]
    layer = pl.program_id(0)
    for n, g_ref in enumerate(gs):

        @pl.when(layer == n)
        def _(g_ref=g_ref):
            g = g_ref[ALL].astype(F32) * factor_ref[0]
            w_out[ALL], m_out[ALL], v_out[ALL] = adamw(w_ref[ALL].astype(F32), m_ref[ALL], v_ref[ALL], g)


def update(factor, w, m, v, gs, blocks):
    layers, rows, columns = w.shape
    block = rows // blocks
    own = pl.BlockSpec((None, block, columns), lambda n, i, factor_ref: (n, i, 0))
    grads = [pl.BlockSpec((block, columns), lambda n, i, factor_ref, one=one: (jnp.where(n == one, i, jnp.where(n < one, 0, blocks - 1)), 0))
             for one in range(layers)]
    return pl.pallas_call(
        _update_kernel,
        grid_spec=pltpu.PrefetchScalarGridSpec(
            num_scalar_prefetch=1,
            grid=(layers, blocks),
            in_specs=[own, own, own, *grads],
            out_specs=[own, own, own],
        ),
        out_shape=[jax.ShapeDtypeStruct(w.shape, BF), jax.ShapeDtypeStruct(w.shape, F32), jax.ShapeDtypeStruct(w.shape, F32)],
        compiler_params=_params("arbitrary", "arbitrary"),
        cost_estimate=_cost(20 * w.size, w, m, v, w, m, v, w),
        name="update",
    )(factor, w, m, v, *gs)


def solution(mesh):
    def step(x, dy, *arrays):
        weights, m, v = (arrays[i : i + 7] for i in (0, 7, 14))
        wq, wk, wv, wo, wg, wu, wd = weights
        layers = wq.shape[0]
        half = HEAD // 2
        angle = jnp.arange(x.shape[1], dtype=F32)[:, None] * THETA ** (-jnp.arange(half, dtype=F32) / half)
        cos, sin = jnp.cos(angle), jnp.sin(angle)
        cos, sin = jnp.concatenate([cos, cos], 1), jnp.concatenate([-sin, sin], 1)

        h, kept = x[0], []
        for n in range(layers):
            a, q, k, v_ = pre(h, wq, wk, wv, n, cos, sin)
            o, lse = attend(q, k, v_)
            mid, b = post(o, wo, n, h)
            kept.append((h, a, q, k, v_, o, lse, mid, b))
            if n < layers - 1:
                h = ff(b, mid, wg, wu, wd, n)

        dh, summed = dy[0], [None] * layers
        for n in reversed(range(layers)):
            h, a, q, k, v_, o, lse, mid, b = kept[n]
            *big, db = ff_bwd(b, dh, wg, wu, wd, n)
            if n:
                big = lax.psum(big, "dp")
            dmid, do, dwo = post_bwd(db, mid, dh, o, wo, n)
            early = [] if n else [_blocks_of(g) for g in big + small]
            dq, dk, dv, *lefts = attend_bwd(q, k, v_, o, do, lse, cos, sin, early, (0, 1, 2) * 2)
            dwq, dwkv, *more = pre_bwd(dq, dk, dv, a, h, dmid, wq, wk, wv, n, n > 0)
            dh = more[0] if more else None
            small = [dwq, dwo, dwkv]
            summed[n] = list(big) + small
        whole, squares = synchronize(lefts + [_blocks_of(g) for g in small], [_blocks_of(g) for g in summed[1][:3]], (0, 1, 2) * 3, (3,) * 6 + (0,) * 3)
        summed = [whole[:3] + whole[6:], summed[1][:3] + whole[3:6]]
        count = sum(w.size for w in weights)
        factor = jnp.minimum(1.0, 0.5 * lax.rsqrt(jnp.sum(squares[0]) / count + 1e-30))

        new = [None] * 7
        for i in (4, 5, 6):
            new[i] = update(factor[None], weights[i], m[i], v[i], [summed[n][i - 4] for n in range(layers)], UPDATE_BLOCKS[i - 4])
        gq, go, gkv = (jnp.stack([summed[n][3 + j] for n in range(layers)]).astype(F32) * factor for j in range(3))
        for i, g in ((0, gq), (1, gkv[:, :, :HEAD]), (2, gkv[:, :, HEAD:]), (3, go)):
            new[i] = adamw(weights[i].astype(F32), m[i], v[i], g)
        return tuple(one[which] for which in range(3) for one in new)

    states, all_of = P(("rep", "dp"), None, None), P(None, None, None)
    return jax.shard_map(
        step,
        mesh=mesh,
        in_specs=(states, states) + (all_of,) * 21,
        out_specs=(P("rep", None, None),) * 21,
        check_vma=False,
    )
```

```python
import functools

import jax
import jax.numpy as jnp
from jax import lax
from jax.experimental import pallas as pl
from jax.experimental.pallas import tpu as pltpu
from jax.sharding import PartitionSpec as P

NEG = -1e30
HIDDEN = 2 * NEG
LOG2E = 1.4426950408889634
HEAD = 128
THETA = 10000
VMEM = 60 * 2**20
STRIP = 512
ALL = ...
BF = jnp.bfloat16
F32 = jnp.float32
NN, NT, TN = (1, 0), (1, 1), (0, 0)

UPDATE_BLOCKS = (4, 4, 4)


def _dot(a, b, ca, cb):
    return lax.dot_general(a, b, (((ca,), (cb,)), ((), ())), preferred_element_type=F32)


def _params(*kinds):
    return pltpu.CompilerParams(dimension_semantics=kinds, vmem_limit_bytes=VMEM)


def _cost(flops, *arrays):
    return pl.CostEstimate(flops=int(flops), transcendentals=0, bytes_accessed=sum(a.size * a.dtype.itemsize for a in arrays))


def _once(shape, index):
    return pl.BlockSpec(shape, index, pipeline_mode=pl.Buffered(1))


def _turn(t, cos, sin):
    return t * cos + pltpu.roll(t, HEAD // 2, 1) * sin


def _scale_of(x):
    return lax.rsqrt(jnp.mean(x * x, -1, keepdims=True) + 1e-6)


def _norm_back(x, d):
    s = _scale_of(x)
    return s * d - x * (s * s * s * jnp.mean(d * x, -1, keepdims=True))


ORDERS = ((1, 8, 4, 2), (1, 4, 2, 8), (1, 2, 8, 4))
BITS = (1, 2, 4, 8)
SCALARS = (2, 1, 4, 8)
TILE = (8, 128)
MESH = pl.DeviceIdType.MESH


def _bit(me, bit):
    return lax.rem(lax.div(me, bit), 2)


def _partner(me, bit):
    return {"dp": me + bit * (1 - 2 * _bit(me, bit))}


def _greet(me):
    barrier = pltpu.get_barrier_semaphore()
    for bit in BITS:
        pl.semaphore_signal(barrier, device_id=_partner(me, bit), device_id_type=MESH)
    pl.semaphore_wait(barrier, len(BITS))


def _squares(x):
    x = x.astype(F32)
    x = (x * x).sum(axis=0, keepdims=True)
    return sum(x[:, at : at + TILE[1]] for at in range(0, x.shape[1], TILE[1]))


class Exchanges:
    def __init__(self, me, streams, mine, buffers, send, recv, local, outs=None):
        self.me, self.streams, self.mine, self.buffers, self.outs = me, streams, mine, buffers, outs
        self.send, self.recv, self.local = send, recv, local
        self.bits = [[_bit(me, bit) for bit in ORDERS[s[2]]] for s in streams]

    def inside(self, n, phase):
        made = max(self.streams[n][3], 1)
        return sum((16 >> (i + 1)) * self.bits[n][i] for i in range(made, phase))

    def block(self, n, phase=4):
        return sum((16 >> (i + 1)) * self.bits[n][i] for i in range(phase))

    def copy(self, n, phase):
        array, columns, group, made = self.streams[n]
        keep, *came = self.buffers[n]
        if phase < 4:
            half = 8 >> phase
            if phase == 0:
                source = self.mine[array].at[pl.ds(half * (1 - self.bits[n][0]), half), :, columns]
            else:
                source = keep.at[pl.ds(self.inside(n, phase) + half * (1 - self.bits[n][phase]), half)]
            target, bit = came[phase - made], ORDERS[group][phase]
        else:
            here = pl.ds(self.block(n, 8 - phase), 1 << (phase - 4))
            source, bit = came[-1].at[here], ORDERS[group][7 - phase]
            target = self.outs[array].at[here, :, columns] if phase == 7 else source
        return pltpu.make_async_remote_copy(src_ref=source, dst_ref=target, send_sem=self.send.at[n, phase], recv_sem=self.recv.at[n, phase],
                                            device_id=_partner(self.me, bit), device_id_type=MESH)

    def load(self, n):
        array, columns, _, made = self.streams[n]
        source = self.mine[array].at[:, :, columns] if made else self.mine[array].at[pl.ds(8 * self.bits[n][0], 8), :, columns]
        return pltpu.make_async_copy(source, self.buffers[n][0], self.local.at[n])

    def store(self, n):
        array, columns, _, _ = self.streams[n]
        here = pl.ds(self.block(n, 1), 8)
        return pltpu.make_async_copy(self.buffers[n][-1].at[here], self.outs[array].at[here, :, columns], self.local.at[n])

    def begin(self, n):
        if not self.streams[n][3]:
            self.copy(n, 0).start()
        self.load(n).start()

    def take(self, n, phase):
        made = self.streams[n][3]
        if phase == made:
            self.load(n).wait()
        self.copy(n, phase).wait_recv()
        keep, came = self.buffers[n][0], self.buffers[n][1 + phase - made]
        at = self.inside(n, phase + 1)

        def one(i, _):
            keep[at + i] = (keep[at + i].astype(F32) + came[i].astype(F32)).astype(BF)

        lax.fori_loop(0, 8 >> phase, one, None)


def _streams(views, groups, made):
    streams = []
    for array, view in enumerate(views):
        rows, width = view.shape[1:]
        cut = width if width * rows < 2**16 else -(-width // 256) * 128
        streams += [(array, slice(at, min(at + cut, width)), groups[array], made[array]) for at in range(0, width, cut)]
    return sorted(streams, key=lambda s: (s[1].start, -views[s[0]].size))


def _blocks_of(g):
    return g.reshape(16, g.shape[0] // 16, g.shape[1])


def _sync_kernel(*refs, streams, many, more):
    mine, others, outs, total = refs[:many], refs[many : many + more], refs[many + more : 2 * many + more], refs[2 * many + more]
    scratch = list(refs[2 * many + more + 1 :])
    blocks = [scratch.pop(0) for _ in range(more)]
    buffers = [[scratch.pop(0) for _ in range(2 + 4 - s[3])] for s in streams]
    sums, send, recv, local, sum_send, sum_recv, block_sem = scratch
    me = lax.axis_index("dp")
    _greet(me)
    x = Exchanges(me, streams, mine, buffers, send, recv, local, outs)
    every = range(len(streams))
    ready = [n for n in every if streams[n][3]]
    fresh = [n for n in every if not streams[n][3]]
    for n in fresh + ready:
        x.begin(n)
    loads = []
    for array in range(more):
        n = [s[0] for s in streams].index(array)
        loads.append(pltpu.make_async_copy(others[array].at[x.block(n)], blocks[array], block_sem.at[array]))
        loads[-1].start()
    for n in ready:
        x.load(n).wait()
        x.copy(n, 3).start()
    part = jnp.zeros((1, TILE[1]), F32)
    for load, block in zip(loads, blocks):
        load.wait()
        part = part + _squares(block[ALL])
    def final(some, part):
        for n in some:
            keep, came, whole = buffers[n][0], buffers[n][-2], buffers[n][-1]
            x.copy(n, 3).wait_recv()
            summed = (keep[x.inside(n, 4)].astype(F32) + came[0].astype(F32)).astype(BF)
            whole[x.block(n)] = summed
            part = part + _squares(summed)
            x.copy(n, 4).start()
        return part

    def onward(some, phase):
        for n in some:
            if phase < 4:
                x.take(n, phase - 1)
            else:
                x.copy(n, phase - 1).wait_recv()
            x.copy(n, phase).start()
            if phase == 7:
                x.store(n).start()

    def scalars(step):
        return pltpu.make_async_remote_copy(src_ref=sums.at[2 * step], dst_ref=sums.at[2 * step + 1], send_sem=sum_send.at[step],
                                            recv_sem=sum_recv.at[step], device_id=_partner(me, SCALARS[step]), device_id_type=MESH)

    def added(step):
        scalars(step).wait_recv()
        sums[2 * step + 2] = sums[2 * step] + sums[2 * step + 1]

    onward(fresh, 1)
    part = final(ready, part)
    onward(fresh, 2)
    onward(fresh, 3)
    part = final(fresh, part)
    sums[0] = jnp.broadcast_to(part, TILE)
    scalars(0).start()
    onward(ready, 5)
    added(0)
    scalars(1).start()
    added(1)
    onward(fresh, 5)
    scalars(2).start()
    onward(ready, 6)
    added(2)
    scalars(3).start()
    onward(fresh, 6)
    onward(ready + fresh, 7)
    added(3)
    total[ALL] = sums[2 * len(BITS)]
    for n in every:
        x.copy(n, 7).wait_recv()
        x.store(n).wait()
        for phase in range(streams[n][3], 8):
            x.copy(n, phase).wait_send()
    for step in range(len(SCALARS)):
        scalars(step).wait_send()


def synchronize(mine, others, groups, made):
    many, more = len(mine), len(others)
    streams = _streams(mine, groups, made)
    scratch = [pltpu.VMEM(v.shape[1:], BF) for v in others]
    for array, columns, _, done in streams:
        first = 16 >> max(done, 1)
        counts = [first] + [8 >> phase for phase in range(done, 4)] + [16]
        scratch += [pltpu.VMEM((count, mine[array].shape[1], columns.stop - columns.start), BF) for count in counts]
    sems = pltpu.SemaphoreType.DMA
    count = len(streams)
    hbm = pl.BlockSpec(memory_space=pl.ANY)
    *outs, total = pl.pallas_call(
        functools.partial(_sync_kernel, streams=streams, many=many, more=more),
        in_specs=[hbm] * (many + more),
        out_specs=[hbm] * many + [pl.BlockSpec(memory_space=pltpu.VMEM)],
        out_shape=[jax.ShapeDtypeStruct((16, *v.shape[1:]), BF) for v in mine] + [jax.ShapeDtypeStruct(TILE, F32)],
        scratch_shapes=scratch + [pltpu.VMEM((2 * len(BITS) + 1, *TILE), F32), sems((count, 8)), sems((count, 8)), sems((count,)),
                                  sems((4,)), sems((4,)), sems((more,))],
        compiler_params=pltpu.CompilerParams(collective_id=0, has_side_effects=True, vmem_limit_bytes=VMEM),
        cost_estimate=_cost(10**9, *mine),
        name="synchronize",
    )(*mine, *others)
    return [o.reshape(-1, o.shape[2]) for o in outs], total


def _pre_kernel(h_ref, wq_ref, wk_ref, wv_ref, cos_ref, sin_ref, a_ref, q_ref, k_ref, v_ref):
    x = h_ref[ALL].astype(F32)
    a = (x * _scale_of(x)).astype(BF)
    a_ref[ALL] = a
    cos, sin = cos_ref[ALL], sin_ref[ALL]

    def turned(t):
        return _turn(t.astype(BF).astype(F32), cos, sin).astype(BF)

    q = _dot(a, wq_ref[ALL], *NN)
    for n in range(q.shape[1] // HEAD):
        q_ref[:, n * HEAD : (n + 1) * HEAD] = turned(q[:, n * HEAD : (n + 1) * HEAD])
    k_ref[ALL] = turned(_dot(a, wk_ref[ALL], *NN))
    v_ref[ALL] = _dot(a, wv_ref[ALL], *NN).astype(BF)


def pre(h, wq, wk, wv, layer, cos, sin, bt=512):
    t, d = h.shape
    rows = lambda w: pl.BlockSpec((bt, w), lambda i: (i, 0))
    weight = lambda w: pl.BlockSpec((None, *w.shape[1:]), lambda i: (layer, 0, 0))
    return pl.pallas_call(
        _pre_kernel,
        grid=(t // bt,),
        in_specs=[rows(d), weight(wq), weight(wk), weight(wv), rows(HEAD), rows(HEAD)],
        out_specs=[rows(d), rows(wq.shape[2]), rows(HEAD), rows(HEAD)],
        out_shape=[jax.ShapeDtypeStruct((t, w), BF) for w in (d, wq.shape[2], HEAD, HEAD)],
        compiler_params=_params("parallel"),
        cost_estimate=_cost(2 * t * d * (wq.shape[2] + 2 * HEAD), h, h, h, h),
        name="attn_pre",
    )(h, wq, wk, wv, cos, sin)


def _gap(bk, cols, bq):
    return lax.rem(lax.broadcasted_iota(jnp.int32, (bk, cols), 1), bq) - lax.broadcasted_iota(jnp.int32, (bk, cols), 0)


def _pieces(g, bq):
    wide = min(STRIP, bq)
    return wide, [(n, at, n * bq + at) for n in range(g) for at in range(0, bq, wide)]


def _attend_kernel(q_ref, k_ref, v_ref, o_ref, lse_ref, top_s, mix_s, gap_s, *, scale, bk):
    bq, g = q_ref.shape[0], q_ref.shape[1] // HEAD
    cols = g * bq
    iq = pl.program_id(0)
    e = scale * LOG2E
    wide, pieces = _pieces(g, bq)

    @pl.when(iq == 0)
    def _():
        gap_s[ALL] = _gap(bk, cols, bq)

    top_s[ALL] = jnp.full((1, cols), NEG, F32)
    mix_s[ALL] = jnp.zeros((HEAD + 8, cols), F32)
    ones = jnp.ones((8, bk), BF)

    def block(j, masked):
        here = pl.ds(pl.multiple_of(j * bk, bk), bk)
        keys = k_ref[here, :]
        scores = [_dot(keys, q_ref[at : at + wide, n * HEAD : (n + 1) * HEAD], *NT) for n, at, _ in pieces]
        weights, keeps = [], []
        for (n, at, c), s in zip(pieces, scores):
            if masked:
                s = jnp.where(gap_s[:, c : c + wide] >= j * bk - iq * bq, s, HIDDEN)
            old = top_s[:, c : c + wide]
            top = jnp.maximum(old, s.max(axis=0, keepdims=True))
            top_s[:, c : c + wide] = top
            weights.append(jnp.exp2((s - top) * e).astype(BF))
            keeps.append(jnp.exp2((old - top) * e))
        values = jnp.concatenate([v_ref[here, :].T, ones], axis=0)
        for (n, at, c), p, keep in zip(pieces, weights, keeps):
            mix_s[:, c : c + wide] = mix_s[:, c : c + wide] * keep + _dot(values, p, *NN)

    whole = lax.div(iq * bq + 1, bk)
    last = lax.div(iq * bq + bq - 1 + bk, bk)
    lax.fori_loop(0, whole, lambda j, _: block(j, False), None)
    lax.fori_loop(whole, last, lambda j, _: block(j, True), None)
    total = mix_s[HEAD : HEAD + 1, :]
    lse = top_s[ALL] * scale + jnp.log(total)
    inv = 1 / total
    for n in range(g):
        c = n * bq
        o_ref[:, n * HEAD : (n + 1) * HEAD] = (mix_s[:HEAD, c : c + bq] * inv[:, c : c + bq]).T.astype(BF)
        lse_ref[n : n + 1, :] = lse[:, c : c + bq]


def attend(q, k, v, bq=512, bk=512):
    t, hd = q.shape
    g = hd // HEAD
    every = pl.BlockSpec((t, HEAD), lambda i: (0, 0))
    return pl.pallas_call(
        functools.partial(_attend_kernel, scale=HEAD**-0.5, bk=bk),
        grid=(t // bq,),
        in_specs=[pl.BlockSpec((bq, hd), lambda i: (i, 0)), every, every],
        out_specs=[pl.BlockSpec((bq, hd), lambda i: (i, 0)), pl.BlockSpec((g, bq), lambda i: (0, i))],
        out_shape=[jax.ShapeDtypeStruct((t, hd), BF), jax.ShapeDtypeStruct((g, t), F32)],
        scratch_shapes=[pltpu.VMEM((1, g * bq), F32), pltpu.VMEM((HEAD + 8, g * bq), F32), pltpu.VMEM((bk, g * bq), jnp.int32)],
        compiler_params=_params("arbitrary"),
        cost_estimate=_cost(8 * g * t * t * HEAD, q, k, v, q),
        name="attend",
    )(q, k, v)


def _attend_bwd_kernel(q_ref, k_ref, v_ref, o_ref, do_ref, lse_ref, cosq_ref, sinq_ref, cos_ref, sin_ref, dq_ref, dk_ref, dv_ref,
                       dq_s, dk_s, dv_s, gap_s, *, scale, bk, hook=None):
    bq, g = q_ref.shape[0], q_ref.shape[1] // HEAD
    cols = g * bq
    iq = pl.program_id(0)
    e = scale * LOG2E
    wide, pieces = _pieces(g, bq)

    @pl.when(iq == 0)
    def _():
        gap_s[ALL] = _gap(bk, cols, bq)
        dk_s[ALL] = jnp.zeros_like(dk_s)
        dv_s[ALL] = jnp.zeros_like(dv_s)

    if hook:
        hook(iq, False)
    dq_s[ALL] = jnp.zeros_like(dq_s)
    lses = [lse_ref[n : n + 1, at : at + wide] * LOG2E for n, at, _ in pieces]
    deltas = []
    for n, at, _ in pieces:
        product = do_ref[at : at + wide, n * HEAD : (n + 1) * HEAD].astype(F32) * o_ref[at : at + wide, n * HEAD : (n + 1) * HEAD].astype(F32)
        deltas.append(product.T.sum(axis=0, keepdims=True))

    def block(j, masked):
        here = pl.ds(pl.multiple_of(j * bk, bk), bk)
        keys, values = k_ref[here, :], v_ref[here, :]
        qs = [q_ref[at : at + wide, n * HEAD : (n + 1) * HEAD] for n, at, _ in pieces]
        dos = [do_ref[at : at + wide, n * HEAD : (n + 1) * HEAD] for n, at, _ in pieces]
        scores = [_dot(keys, x, *NT) for x in qs]
        dps = [_dot(values, x, *NT) for x in dos]
        keys_t = keys.T
        for i, (n, at, c) in enumerate(pieces):
            p = jnp.exp2(scores[i] * e - lses[i])
            if masked:
                p = jnp.where(gap_s[:, c : c + wide] >= j * bk - iq * bq, p, 0.0)
            ds = (p * (dps[i] - deltas[i])).astype(BF)
            dv_s[here, :] += _dot(p.astype(BF), dos[i], *NN)
            dk_s[here, :] += _dot(ds, qs[i], *NN)
            dq_s[:, c : c + wide] += _dot(keys_t, ds, *NN)

    whole = lax.div(iq * bq + 1, bk)
    last = lax.div(iq * bq + bq - 1 + bk, bk)
    lax.fori_loop(0, whole, lambda j, _: block(j, False), None)
    lax.fori_loop(whole, last, lambda j, _: block(j, True), None)
    for n in range(g):
        d = (dq_s[:, n * bq : (n + 1) * bq] * scale).T.astype(BF).astype(F32)
        dq_ref[:, n * HEAD : (n + 1) * HEAD] = _turn(d, cosq_ref[ALL], -sinq_ref[ALL]).astype(BF)

    @pl.when(iq == pl.num_programs(0) - 1)
    def _():
        d = (dk_s[ALL] * scale).astype(BF).astype(F32)
        dk_ref[ALL] = _turn(d, cos_ref[ALL], -sin_ref[ALL]).astype(BF)
        dv_ref[ALL] = dv_s[ALL].astype(BF)

    if hook:
        hook(iq, True)


def _attend_bwd_sync_kernel(*refs, streams, many, scale, bk):
    given, mine, results, lefts, scratch = refs[:10], refs[10 : 10 + many], refs[10 + many : 13 + many], refs[13 + many : 13 + 2 * many], refs[13 + 2 * many :]
    own, scratch = scratch[:4], list(scratch[4:])
    buffers = [[scratch.pop(0) for _ in range(4)] for _ in streams]
    me = lax.axis_index("dp")
    x = Exchanges(me, streams, mine, buffers, *scratch)
    every = range(len(streams))
    early = [n for n in every if n < 3]
    late = [n for n in every if n >= 3]

    def hook(step, after):
        if after:

            @pl.when(step == HOOKS[3])
            def _():
                for n in every:
                    array, columns, _, _ = streams[n]
                    x.take(n, 2)
                    lefts[array][:, :, columns] = buffers[n][0][pl.ds(x.inside(n, 3), 2)]
                for n in every:
                    for phase in range(3):
                        x.copy(n, phase).wait_send()

            return

        @pl.when(step == 0)
        def _():
            _greet(me)
            for n in every:
                x.begin(n)

        for place, phase, some in ((0, 0, early), (1, 0, late), (2, 1, every)):

            @pl.when(step == HOOKS[place])
            def _(phase=phase, some=some):
                for n in some:
                    x.take(n, phase)
                    x.copy(n, phase + 1).start()

    _attend_bwd_kernel(*given, *results, *own, scale=scale, bk=bk, hook=hook)


HOOKS = (3, 4, 7, 7)


def attend_bwd(q, k, v, o, do, lse, cos, sin, mine=(), groups=(), bq=256, bk=512):
    t, hd = q.shape
    g = hd // HEAD
    every = pl.BlockSpec((t, HEAD), lambda i: (0, 0))
    some = pl.BlockSpec((bq, hd), lambda i: (i, 0))
    table = pl.BlockSpec((bq, HEAD), lambda i: (i, 0))
    kernel, name, params, many = functools.partial(_attend_bwd_kernel, scale=HEAD**-0.5, bk=bk), "attend_bwd", _params("arbitrary"), len(mine)
    scratch = [pltpu.VMEM((HEAD, g * bq), F32), pltpu.VMEM((t, HEAD), F32), pltpu.VMEM((t, HEAD), F32), pltpu.VMEM((bk, g * bq), jnp.int32)]
    if mine:
        streams = _streams(mine, groups, [0] * many)
        kernel = functools.partial(_attend_bwd_sync_kernel, streams=streams, many=many, scale=HEAD**-0.5, bk=bk)
        name = "attend_bwd_sync"
        params = pltpu.CompilerParams(dimension_semantics=("arbitrary",), collective_id=1, has_side_effects=True, vmem_limit_bytes=VMEM)
        for array, columns, _, _ in streams:
            scratch += [pltpu.VMEM((count, mine[array].shape[1], columns.stop - columns.start), BF) for count in (8, 8, 4, 2)]
        sems = pltpu.SemaphoreType.DMA
        scratch += [sems((len(streams), 3)), sems((len(streams), 3)), sems((len(streams),))]
    lefts = [jax.ShapeDtypeStruct((2, *g.shape[1:]), BF) for g in mine]
    return pl.pallas_call(
        kernel,
        grid=(t // bq,),
        in_specs=[some, every, every, some, some, pl.BlockSpec((g, bq), lambda i: (0, i)), table, table, every, every]
        + [pl.BlockSpec(memory_space=pl.ANY)] * many,
        out_specs=[some, every, every] + [_once(left.shape, lambda i: (0, 0, 0)) for left in lefts],
        out_shape=[jax.ShapeDtypeStruct((t, w), BF) for w in (hd, HEAD, HEAD)] + lefts,
        scratch_shapes=scratch,
        compiler_params=params,
        cost_estimate=_cost(14 * g * t * t * HEAD, q, q, q, q),
        name=name,
    )(q, k, v, o, do, lse, cos, sin, cos, sin, *mine)


def _post_kernel(o_ref, wo_ref, h_ref, mid_ref, b_ref):
    mid = h_ref[ALL] + _dot(o_ref[ALL], wo_ref[ALL], *NN).astype(BF)
    mid_ref[ALL] = mid
    x = mid.astype(F32)
    b_ref[ALL] = (x * _scale_of(x)).astype(BF)


def post(o, wo, layer, h, bt=512):
    t, d = h.shape
    rows = lambda w: pl.BlockSpec((bt, w), lambda i: (i, 0))
    return pl.pallas_call(
        _post_kernel,
        grid=(t // bt,),
        in_specs=[rows(o.shape[1]), pl.BlockSpec((None, *wo.shape[1:]), lambda i: (layer, 0, 0)), rows(d)],
        out_specs=[rows(d), rows(d)],
        out_shape=[jax.ShapeDtypeStruct((t, d), BF)] * 2,
        compiler_params=_params("parallel"),
        cost_estimate=_cost(2 * t * d * d, h, h, h, h),
        name="attn_post",
    )(o, wo, h)


def _post_bwd_kernel(db_ref, mid_ref, dh_ref, o_ref, wo_ref, dmid_ref, do_ref, dwo_ref, acc):
    i = pl.program_id(0)
    dx = _norm_back(mid_ref[ALL].astype(F32), db_ref[ALL].astype(F32)).astype(BF)
    dmid = dh_ref[ALL] + dx
    dmid_ref[ALL] = dmid
    do_ref[ALL] = _dot(dmid, wo_ref[ALL], *NT).astype(BF)
    part = _dot(o_ref[ALL], dmid, *TN)

    @pl.when(i == 0)
    def _():
        acc[ALL] = part

    @pl.when(i > 0)
    def _():
        acc[ALL] += part

    @pl.when(i == pl.num_programs(0) - 1)
    def _():
        dwo_ref[ALL] = acc[ALL].astype(BF)


def post_bwd(db, mid, dh, o, wo, layer, bt=512):
    t, d = dh.shape
    rows = lambda w: pl.BlockSpec((bt, w), lambda i: (i, 0))
    return pl.pallas_call(
        _post_bwd_kernel,
        grid=(t // bt,),
        in_specs=[rows(d), rows(d), rows(d), rows(o.shape[1]), pl.BlockSpec((None, *wo.shape[1:]), lambda i: (layer, 0, 0))],
        out_specs=[rows(d), rows(o.shape[1]), pl.BlockSpec(wo.shape[1:], lambda i: (0, 0))],
        out_shape=[jax.ShapeDtypeStruct((t, d), BF), jax.ShapeDtypeStruct(o.shape, BF), jax.ShapeDtypeStruct(wo.shape[1:], BF)],
        scratch_shapes=[pltpu.VMEM(wo.shape[1:], F32)],
        compiler_params=_params("arbitrary"),
        cost_estimate=_cost(4 * t * d * d, dh, dh, dh, dh, dh, dh),
        name="attn_post_bwd",
    )(db, mid, dh, o, wo)


def _pre_bwd_kernel(dq_ref, dk_ref, dv_ref, a_ref, *rest, further):
    if further:
        h_ref, dmid_ref, wq_ref, wk_ref, wv_ref, dwq_ref, dwkv_ref, dh_ref, acc = rest
    else:
        dwq_ref, dwkv_ref, acc = rest
    i = pl.program_id(0)
    dq, dk, dv = dq_ref[ALL], dk_ref[ALL], dv_ref[ALL]
    part = _dot(a_ref[ALL], jnp.concatenate([dq, dk, dv], axis=1), *TN)

    @pl.when(i == 0)
    def _():
        acc[ALL] = part

    @pl.when(i > 0)
    def _():
        acc[ALL] += part

    @pl.when(i == pl.num_programs(0) - 1)
    def _():
        wide = dwq_ref.shape[1]
        dwq_ref[ALL] = acc[:, :wide].astype(BF)
        dwkv_ref[ALL] = acc[:, wide:].astype(BF)

    if further:
        da = (_dot(dq, wq_ref[ALL], *NT) + _dot(dk, wk_ref[ALL], *NT) + _dot(dv, wv_ref[ALL], *NT)).astype(BF).astype(F32)
        dh_ref[ALL] = dmid_ref[ALL] + _norm_back(h_ref[ALL].astype(F32), da).astype(BF)


def pre_bwd(dq, dk, dv, a, h, dmid, wq, wk, wv, layer, further, bt=512):
    t, d = a.shape
    wide = dq.shape[1]
    rows = lambda w: pl.BlockSpec((bt, w), lambda i: (i, 0))
    weight = lambda w: pl.BlockSpec((None, *w.shape[1:]), lambda i: (layer, 0, 0))
    given = [dq, dk, dv, a]
    specs = [rows(wide), rows(HEAD), rows(HEAD), rows(d)]
    outs = [jax.ShapeDtypeStruct((d, wide), BF), jax.ShapeDtypeStruct((d, 2 * HEAD), BF)]
    out_specs = [pl.BlockSpec(s.shape, lambda i: (0, 0)) for s in outs]
    if further:
        given += [h, dmid, wq, wk, wv]
        specs += [rows(d), rows(d), weight(wq), weight(wk), weight(wv)]
        outs.append(jax.ShapeDtypeStruct((t, d), BF))
        out_specs.append(rows(d))
    return pl.pallas_call(
        functools.partial(_pre_bwd_kernel, further=further),
        grid=(t // bt,),
        in_specs=specs,
        out_specs=out_specs,
        out_shape=outs,
        scratch_shapes=[pltpu.VMEM((d, wide + 2 * HEAD), F32)],
        compiler_params=_params("arbitrary"),
        cost_estimate=_cost((4 if further else 2) * t * d * (wide + 2 * HEAD), a, a, a, a),
        name="attn_pre_bwd",
    )(*given)


def _silu(g):
    s = 1 / (1 + jnp.exp(-g))
    return s, g * s


def _ff_kernel(b_ref, mid_ref, wg_ref, wu_ref, wd_ref, out_ref, gate_ref, up_ref, *, chunk):
    b = b_ref[ALL]
    width = wg_ref.shape[1]
    total = None
    for at in range(0, width, chunk):
        f = slice(at, min(at + chunk, width))
        gate, up = _dot(b, wg_ref[:, f], *NN), _dot(b, wu_ref[:, f], *NN)
        gate_ref[:, f], up_ref[:, f] = gate, up
        act = (_silu(gate)[1] * up).astype(BF)
        part = _dot(act, wd_ref[f, :], *NN)
        total = part if total is None else total + part
    out_ref[ALL] = mid_ref[ALL] + total.astype(BF)


def ff(b, mid, wg, wu, wd, layer, bt=256, chunk=768):
    t, d = b.shape
    hidden = wg.shape[2]
    rows = pl.BlockSpec((bt, d), lambda i: (i, 0))
    weight = lambda w: _once((None, *w.shape[1:]), lambda i: (layer, 0, 0))
    return pl.pallas_call(
        functools.partial(_ff_kernel, chunk=chunk),
        grid=(t // bt,),
        in_specs=[rows, rows, weight(wg), weight(wu), weight(wd)],
        out_specs=[rows] + [pl.BlockSpec((bt, hidden), lambda i: (i, 0))] * 2,
        out_shape=[jax.ShapeDtypeStruct((t, d), BF)] + [jax.ShapeDtypeStruct((t, hidden), F32)] * 2,
        compiler_params=_params("parallel"),
        cost_estimate=_cost(6 * t * d * wg.shape[2], b, b, b, wg, wu),
        name="ff",
    )(b, mid, wg, wu, wd)


def _ff_bwd_kernel(b_ref, dh_ref, wg_ref, wu_ref, wd_ref, *rest, saved, **sizes):
    kept, rest = (rest[:2], rest[2:]) if saved else ((), rest)
    _ff_bwd_body(kept, b_ref, dh_ref, wg_ref, wu_ref, wd_ref, *rest, **sizes)


def _ff_bwd_body(kept, b_ref, dh_ref, wg_ref, wu_ref, wd_ref, dwg_ref, dwu_ref, dwd_ref, db_ref, bt_s, dht_s, act_s, dg_s, du_s, acc, *, width, tb):
    j = pl.program_id(0)
    t, block = b_ref.shape[0], wg_ref.shape[1]
    left = width - j * block

    @pl.when(j == 0)
    def _():
        bt_s[ALL] = b_ref[ALL].T
        dht_s[ALL] = dh_ref[ALL].T
        acc[ALL] = jnp.zeros_like(acc)

    across = lax.broadcasted_iota(jnp.int32, (1, block), 1) < left
    down = lax.broadcasted_iota(jnp.int32, (block, 1), 0) < left
    zero = jnp.zeros((), BF)
    wg, wu, wd = jnp.where(across, wg_ref[ALL], zero), jnp.where(across, wu_ref[ALL], zero), jnp.where(down, wd_ref[ALL], zero)
    for at in range(0, t, tb):
        here = slice(at, at + tb)
        b, dh = b_ref[here, :], dh_ref[here, :]
        g, u = [jnp.where(across, ref[here, :], 0.0) for ref in kept] if kept else (_dot(b, wg, *NN), _dot(b, wu, *NN))
        da = _dot(dh, wd, *NT).astype(BF).astype(F32)
        s, silu = _silu(g)
        act_s[here, :] = (silu * u).astype(BF)
        du = (da * silu).astype(BF)
        dg = (da * u * (s + silu * (1 - s))).astype(BF)
        du_s[here, :] = du
        dg_s[here, :] = dg
        acc[here, :] += _dot(dg, wg, *NT) + _dot(du, wu, *NT)
    dwg_ref[ALL] = _dot(bt_s[ALL], dg_s[ALL], *NN).astype(BF)
    dwu_ref[ALL] = _dot(bt_s[ALL], du_s[ALL], *NN).astype(BF)
    dwd_ref[ALL] = _dot(dht_s[ALL], act_s[ALL], *NN).T.astype(BF)

    @pl.when(j == pl.num_programs(0) - 1)
    def _():
        db_ref[ALL] = acc[ALL].astype(BF)


def ff_bwd(b, dh, wg, wu, wd, layer, kept=(), block=512, tb=512):
    t, d = b.shape
    width = wg.shape[2]
    every = _once((t, d), lambda j: (0, 0))
    columns = pl.BlockSpec((None, d, block), lambda j: (layer, 0, j))
    out_columns = pl.BlockSpec((d, block), lambda j: (0, j))
    return pl.pallas_call(
        functools.partial(_ff_bwd_kernel, saved=bool(kept), width=width, tb=tb),
        grid=(-(-width // block),),
        in_specs=[every, every, columns, columns, pl.BlockSpec((None, block, d), lambda j: (layer, j, 0))]
        + [pl.BlockSpec((t, block), lambda j: (0, j))] * len(kept),
        out_specs=[out_columns, out_columns, pl.BlockSpec((block, d), lambda j: (j, 0)), _once((t, d), lambda j: (0, 0))],
        out_shape=[jax.ShapeDtypeStruct((d, width), BF), jax.ShapeDtypeStruct((d, width), BF), jax.ShapeDtypeStruct((width, d), BF),
                   jax.ShapeDtypeStruct((t, d), BF)],
        scratch_shapes=[pltpu.VMEM((d, t), BF), pltpu.VMEM((d, t), BF)] + [pltpu.VMEM((t, block), BF)] * 3 + [pltpu.VMEM((t, d), F32)],
        compiler_params=_params("arbitrary"),
        cost_estimate=_cost((12 if kept else 16) * t * d * width, b, dh, wg, wu, wd, *kept),
        name="ff_bwd",
    )(b, dh, wg, wu, wd, *kept)


def adamw(w, m, v, g):
    m = 0.9 * m + 0.1 * g
    v = 0.95 * v + 0.05 * g * g
    step = m * lax.rsqrt(v + 1e-8) + 0.1 * w
    return (w - 0.02 * step).astype(BF), m, v


def _update_kernel(factor_ref, w_ref, m_ref, v_ref, *rest):
    gs, (w_out, m_out, v_out) = rest[:-3], rest[-3:]
    layer = pl.program_id(0)
    for n, g_ref in enumerate(gs):

        @pl.when(layer == n)
        def _(g_ref=g_ref):
            g = g_ref[ALL].astype(F32) * factor_ref[0]
            w_out[ALL], m_out[ALL], v_out[ALL] = adamw(w_ref[ALL].astype(F32), m_ref[ALL], v_ref[ALL], g)


def update(factor, w, m, v, gs, blocks):
    layers, rows, columns = w.shape
    block = rows // blocks
    own = pl.BlockSpec((None, block, columns), lambda n, i, factor_ref: (n, i, 0))
    grads = [pl.BlockSpec((block, columns), lambda n, i, factor_ref, one=one: (jnp.where(n == one, i, jnp.where(n < one, 0, blocks - 1)), 0))
             for one in range(layers)]
    return pl.pallas_call(
        _update_kernel,
        grid_spec=pltpu.PrefetchScalarGridSpec(
            num_scalar_prefetch=1,
            grid=(layers, blocks),
            in_specs=[own, own, own, *grads],
            out_specs=[own, own, own],
        ),
        out_shape=[jax.ShapeDtypeStruct(w.shape, BF), jax.ShapeDtypeStruct(w.shape, F32), jax.ShapeDtypeStruct(w.shape, F32)],
        compiler_params=_params("arbitrary", "arbitrary"),
        cost_estimate=_cost(20 * w.size, w, m, v, w, m, v, w),
        name="update",
    )(factor, w, m, v, *gs)


def solution(mesh):
    def step(x, dy, *arrays):
        weights, m, v = (arrays[i : i + 7] for i in (0, 7, 14))
        wq, wk, wv, wo, wg, wu, wd = weights
        layers = wq.shape[0]
        half = HEAD // 2
        angle = jnp.arange(x.shape[1], dtype=F32)[:, None] * THETA ** (-jnp.arange(half, dtype=F32) / half)
        cos, sin = jnp.cos(angle), jnp.sin(angle)
        cos, sin = jnp.concatenate([cos, cos], 1), jnp.concatenate([-sin, sin], 1)

        h, kept = x[0], []
        for n in range(layers):
            a, q, k, v_ = pre(h, wq, wk, wv, n, cos, sin)
            o, lse = attend(q, k, v_)
            mid, b = post(o, wo, n, h)
            projections = []
            kept.append((h, a, q, k, v_, o, lse, mid, b, projections))
            if n < layers - 1:
                h, *projections[:] = ff(b, mid, wg, wu, wd, n)

        dh, summed = dy[0], [None] * layers
        for n in reversed(range(layers)):
            h, a, q, k, v_, o, lse, mid, b, projections = kept[n]
            *big, db = ff_bwd(b, dh, wg, wu, wd, n, projections)
            if n:
                big = lax.psum(big, "dp")
            dmid, do, dwo = post_bwd(db, mid, dh, o, wo, n)
            early = [] if n else [_blocks_of(g) for g in big + small]
            dq, dk, dv, *lefts = attend_bwd(q, k, v_, o, do, lse, cos, sin, early, (0, 1, 2) * 2, bq=512 if n else 256)
            dwq, dwkv, *more = pre_bwd(dq, dk, dv, a, h, dmid, wq, wk, wv, n, n > 0)
            dh = more[0] if more else None
            small = [dwq, dwo, dwkv]
            summed[n] = list(big) + small
        whole, squares = synchronize(lefts + [_blocks_of(g) for g in small], [_blocks_of(g) for g in summed[1][:3]], (0, 1, 2) * 3, (3,) * 6 + (0,) * 3)
        summed = [whole[:3] + whole[6:], summed[1][:3] + whole[3:6]]
        count = sum(w.size for w in weights)
        factor = jnp.minimum(1.0, 0.5 * lax.rsqrt(jnp.sum(squares[0]) / count + 1e-30))

        new = [None] * 7
        for i in (4, 5, 6):
            new[i] = update(factor[None], weights[i], m[i], v[i], [summed[n][i - 4] for n in range(layers)], UPDATE_BLOCKS[i - 4])
        gq, go, gkv = (jnp.stack([summed[n][3 + j] for n in range(layers)]).astype(F32) * factor for j in range(3))
        for i, g in ((0, gq), (1, gkv[:, :, :HEAD]), (2, gkv[:, :, HEAD:]), (3, go)):
            new[i] = adamw(weights[i].astype(F32), m[i], v[i], g)
        return tuple(one[which] for which in range(3) for one in new)

    states, all_of = P(("rep", "dp"), None, None), P(None, None, None)
    return jax.shard_map(
        step,
        mesh=mesh,
        in_specs=(states, states) + (all_of,) * 21,
        out_specs=(P("rep", None, None),) * 21,
        check_vma=False,
    )
```
